128 devices in a mesh: dp: 4 (over y), vocab: 32 (over z, x, core).
Axes of the slice: x: 4, y: 4, z: 4, core: 2. Of those that a mesh axis runs over, the one named last changes fastest.
Arguments:
- input_ids: int32 [1024], P('dp'), may hold values from 0 to 255999
- target_ids: int32 [1024], P('dp'), may hold values from 0 to 255999
- loss_mask: int32 [1024], P('dp'), may hold values 0 or 1
- final_hidden: bfloat16 [1024, 3584], P('dp'), may hold values from -5 to 5, as said below
- norm_gain: float32 [3584], replicated, may hold values from 0.25 to 1.75
- embed_cotangent: bfloat16 [1024, 3584], P('dp'), may hold values from -0.059814453 to 0.059814453
- table: bfloat16 [256000, 3584], P(('dp', 'vocab')), may hold values from -0.08351914 to 0.08351914, as said below
Outputs:
- embedded: bfloat16 [1024, 3584], P('dp')
- loss: float32 [], replicated
- grad_hidden: bfloat16 [1024, 3584], P('dp')
- gain_grad: float32 [3584], replicated
- table_grad: bfloat16 [256000, 3584], P(('dp', 'vocab'))
The draws below stay inside these ranges and needn't reach their ends.
Inputs may be any that keep to these rules, and one draw needn't show every extreme that they name: Every entry of table lies within -5 / sqrt(3584) and 5 / sqrt(3584). Every entry of final_hidden lies within -5 and 5.
All inputs are finite; a program needn't handle non-finite values.
Results may differ from the reference program's by a relative error of at most 0.003.
Values may be sent and summed in bfloat16 or wider, within the bound.
A program may use at most 256 MiB of HBM per device.

```python
import math
import jax
import jax.numpy as jnp
import numpy as np
from jax import lax

D = 3584
SOFTCAP = 30
ROWS = 2000
V = 256000
TOKENS = 1024
N_DP = 4
N_VOCAB = 32


def hub_layout(key):
    hub_stride = ROWS // 4
    hub_count = V // hub_stride
    unit_scale = 1.0 / math.sqrt(D)
    directions = jax.random.truncated_normal(jax.random.fold_in(key, 701), -4.0, 4.0, (hub_count, D), jnp.float32) * unit_scale
    return (hub_stride, hub_count, directions)


def draw_table(key, part):
    hub_stride, hub_count, directions = hub_layout(key)
    unit_scale = 1.0 / math.sqrt(D)
    noise_rows = jax.random.truncated_normal(jax.random.fold_in(key, 703), -4.0, 4.0, (V, D), jnp.float32)
    blocks = (noise_rows * unit_scale).reshape(hub_count, hub_stride, D)
    blocks = blocks.at[:, 0, :].add(directions)
    return jnp.clip(blocks.reshape(V, D), -5.0 * unit_scale, 5.0 * unit_scale).astype(jnp.bfloat16)


def draw_final_hidden(key, part):
    hub_stride, hub_count, directions = hub_layout(key)
    topics = jax.random.randint(jax.random.fold_in(key, 709), (TOKENS,), 0, hub_count)
    leaning = jax.random.uniform(jax.random.fold_in(key, 711), (TOKENS, 1), jnp.float32, 0.1, 0.45)
    base_rows = jax.random.truncated_normal(jax.random.fold_in(key, 713), -4.0, 4.0, (TOKENS, D), jnp.float32)
    pointed = jnp.take(directions, topics, axis=0) * math.sqrt(D)
    return jnp.clip(base_rows + leaning * pointed, -5.0, 5.0).astype(jnp.bfloat16)


def set_ends(entries, rng, low, high):
    shape = entries.shape
    index_at = [jax.random.randint(jax.random.fold_in(rng, axis), (), 0, shape[axis]) for axis in range(len(shape))]
    entries = entries.at[tuple(index_at)].set(low)
    longest = shape.index(max(shape))
    index_at[longest] = (index_at[longest] + 1) % shape[longest]
    return entries.at[tuple(index_at)].set(high)


def levels(rng, shape, pieces, smallest, largest):
    loudness, own = 1.0, jax.random.fold_in(rng, 6)
    for axis_at, blocks in pieces:
        steps = jnp.exp(jax.random.uniform(jax.random.fold_in(own, axis_at), (blocks,), jnp.float32, smallest / len(pieces), largest / len(pieces)))
        loudness = loudness * jnp.repeat(steps, shape[axis_at] // blocks).reshape([-1 if axis == axis_at else 1 for axis in range(len(shape))])
    return loudness


def ranked_wide(own_key, dims, count, skew):
    portions = [min(1 << octave, count + 1 - (1 << octave)) * (1 << 20) // math.isqrt((1 << octave) ** skew) + 1 for octave in range((count + 1).bit_length()) if 1 << octave <= count]
    spread = 1 + sum(portions) // (1 << 30)
    listing = np.cumsum(np.array([max(1, weight // spread) for weight in portions]))
    lot = jax.random.randint(jax.random.fold_in(own_key, 1), dims, 0, int(listing[len(portions) - 1]))
    start = jnp.left_shift(1, jnp.searchsorted(jnp.asarray(listing, jnp.int32), lot, side="right").astype(jnp.int32))
    rank = start - 1 + jax.random.randint(jax.random.fold_in(own_key, 4), dims, 0, 1 << 30) % jnp.minimum(start, count + 1 - start)
    return jax.random.permutation(jax.random.fold_in(own_key, 2), count)[rank].astype(jnp.int32)


def gaussian(stream_key, shape, deviation, limit, cuts=(), kind=jnp.bfloat16):
    gain = levels(stream_key, shape, cuts, -0.22, 0.18) if cuts else 1.0
    array = jax.random.normal(stream_key, shape, jnp.float32) * deviation * gain
    return jnp.minimum(jnp.maximum(array, -limit), limit).astype(kind)


def setup_inputs(seed: int = 0) -> dict:
    keys = jax.random.split(jax.random.key(seed), 8)
    input_ids = set_ends(ranked_wide(keys[0], (TOKENS,), V, 2), jax.random.fold_in(keys[0], 3), 0, V - 1).astype(jnp.int32)
    target_ids = set_ends(ranked_wide(keys[1], (TOKENS,), V, 2), jax.random.fold_in(keys[1], 3), 0, V - 1).astype(jnp.int32)
    loss_mask = set_ends((jax.random.randint(keys[2], (TOKENS,), 0, 8) < 7).astype(jnp.int32), jax.random.fold_in(keys[2], 1), 0, 1)
    final_hidden = draw_final_hidden(jax.random.fold_in(keys[7], 71), 0)
    norm_gain = jnp.clip(1.0 + 0.15 * jax.random.normal(keys[4], (D,), jnp.float32), 0.25, 1.75)
    embed_cotangent = gaussian(keys[5], (TOKENS, D), 0.01, 0.059814453, ((0, 4),))
    table = draw_table(jax.random.fold_in(keys[7], 71), 0)
    return dict(input_ids=input_ids, target_ids=target_ids, loss_mask=loss_mask, final_hidden=final_hidden, norm_gain=norm_gain, embed_cotangent=embed_cotangent, table=table)


EPSILON = 1e-06

def norm_backward(upstream, widened, inv_rms, norm_gain):
    scaled_up = upstream * norm_gain
    mean_dot = lax.optimization_barrier(jnp.mean(scaled_up * widened, axis=1, keepdims=True))
    gradient = inv_rms * scaled_up - widened * (inv_rms * inv_rms * inv_rms) * mean_dot
    gain_part = lax.optimization_barrier(jnp.sum(upstream * widened * inv_rms, axis=0))
    return (gradient.astype(jnp.bfloat16), gain_part)

def reference(input_ids, target_ids, loss_mask, final_hidden, norm_gain, embed_cotangent, table):
    block_count = N_DP * N_VOCAB
    block_rows = V // block_count
    embed_scale = math.sqrt(D)
    embedded = (jnp.take(table, input_ids, axis=0).astype(jnp.float32) * embed_scale).astype(jnp.bfloat16)
    widened = final_hidden.astype(jnp.float32)
    inv_rms = lax.rsqrt(lax.optimization_barrier(jnp.mean(widened * widened, axis=1, keepdims=True)) + EPSILON)
    normed = (widened * inv_rms * norm_gain).astype(jnp.bfloat16)
    blocks = table.reshape(block_count, block_rows, D)
    starts = (jnp.arange(block_count) * block_rows).astype(jnp.int32)

    def forward_block(rows_block):
        raw_logits = jnp.dot(normed, rows_block.T, preferred_element_type=jnp.float32)
        return SOFTCAP * jnp.tanh(raw_logits / SOFTCAP)
    capped = lax.map(forward_block, blocks)
    sum_exp = lax.optimization_barrier(jnp.sum(jnp.exp(capped), axis=(0, 2)))
    token_weight = loss_mask.astype(jnp.float32)
    cotangent_wide = embed_cotangent.astype(jnp.float32)

    def backward_block(carry, operands):
        upstream, picked = carry
        rows_block, start, capped_block = operands
        local_targets = (target_ids - start).astype(jnp.int32)
        target_hit = lax.broadcasted_iota(jnp.int32, capped_block.shape, 1) == local_targets[:, None]
        picked = picked + lax.optimization_barrier(jnp.sum(jnp.where(target_hit, capped_block, 0.0), axis=1))
        slope = token_weight[:, None] * (jnp.exp(capped_block) / sum_exp[:, None] - target_hit.astype(jnp.float32)) * (1.0 - (capped_block / SOFTCAP) ** 2)
        slope_low = slope.astype(jnp.bfloat16)
        upstream = upstream + jnp.dot(slope_low, rows_block, preferred_element_type=jnp.float32)
        head_part = lax.dot_general(slope_low, normed, (((0,), (0,)), ((), ())), preferred_element_type=jnp.float32)
        local_ids = (input_ids - start).astype(jnp.int32)
        inside = (local_ids >= 0) & (local_ids < block_rows)
        segment_ids = jnp.where(inside, local_ids, block_rows).astype(jnp.int32)
        embed_part = jax.ops.segment_sum(cotangent_wide, segment_ids, num_segments=block_rows + 1)[:block_rows] * embed_scale
        return ((upstream, picked), (head_part + embed_part).astype(jnp.bfloat16))
    initial = (jnp.zeros((TOKENS, D), jnp.float32), jnp.zeros((TOKENS,), jnp.float32))
    (upstream, picked), grad_blocks = lax.scan(backward_block, initial, (blocks, starts, capped))
    loss = jnp.sum(token_weight * (jnp.log(sum_exp) - picked)) / jnp.maximum(jnp.sum(token_weight), 1.0)
    grad_hidden, gain_grad = norm_backward(upstream, widened, inv_rms, norm_gain)
    table_grad = grad_blocks.reshape(V, D)
    return (embedded, loss, grad_hidden, gain_grad, table_grad)
```

```python
import functools
import math

import jax
import jax.numpy as jnp
from jax import lax
from jax.experimental import pallas as pl
from jax.experimental.pallas import tpu as pltpu
from jax.sharding import PartitionSpec as P

SOFTCAP = 30
EPSILON = 1e-06
LANES = 128
F32, BF16, I16, I32 = jnp.float32, jnp.bfloat16, jnp.int16, jnp.int32

SIDE = 4
WIDE = 256
FULL = 32000.0
ORDERS = ((0, 2, 1), (2, 1, 0), (1, 0, 2))


def of(value, step):
    return value if isinstance(value, int) else pl.multiple_of(value, step)


def odd(j):
    return j % 2 if isinstance(j, int) else lax.rem(j, 2)


class Here:
    def __init__(self):
        self.y = lax.axis_index("dp")
        self.v = lax.axis_index("vocab")
        self.z = lax.div(self.v, 8)
        self.x = lax.rem(lax.div(self.v, 2), SIDE)
        self.c = lax.rem(self.v, 2)
        self.co = (self.y, self.z, self.x)
        self.near = [[p] + [lax.rem(p + s, SIDE) for s in (1, 2, 3)] for p in self.co]

    def peer(self, axis, step):
        if axis == 0:
            return {"dp": lax.rem(self.y + step, SIDE)}
        if axis == 1:
            return {"vocab": lax.rem(self.z + step, SIDE) * 8 + lax.rem(self.v, 8)}
        if axis == 2:
            return {"vocab": self.z * 8 + lax.rem(self.x + step, SIDE) * 2 + self.c}
        return {"vocab": self.v + 1 - 2 * self.c}

    def plus(self, axis, step):
        return self.near[axis][step]

    def enter(self, *groups):
        barrier = pltpu.get_barrier_semaphore()
        peers = [peer for group in groups for peer in group]
        for peer in peers:
            pl.semaphore_signal(barrier, inc=1, device_id=peer)
        pl.semaphore_wait(barrier, len(peers))

    def row(self):
        out = []
        for i in range(1, 8):
            x = self.near[2][i // 2]
            out.append({"vocab": self.z * 8 + x * 2 + (1 - self.c if i % 2 else self.c)})
        return out

    def face(self):
        out = []
        for i in range(1, 16):
            z = self.near[1][i % 4]
            out.append({"dp": self.near[0][i // 4], "vocab": z * 8 + lax.rem(self.v, 8)})
        return out

    def axes(self):
        return [self.peer(a, s) for a in range(3) for s in (1, 2, 3)]


class Lanes:
    def __init__(self, send, recv):
        self.send, self.recv, self.made = send, recv, []

    def go(self, ends):
        self.made.append(Trip(self, len(self.made), ends))
        return self.made[-1]


class Trip:
    def __init__(self, lanes, i, ends):
        self.lanes, self.i, self.ends, self.gone = lanes, i, ends, False

    def make(self):
        src, dst, device = self.ends()
        return pltpu.make_async_remote_copy(
            src_ref=src,
            dst_ref=dst,
            send_sem=self.lanes.send.at[self.i],
            recv_sem=self.lanes.recv.at[self.i],
            device_id=device,
        )

    def start(self):
        self.gone = True
        self.make().start()

    def wait_recv(self):
        self.make().wait_recv()

    def wait_send(self):
        self.make().wait_send()


class Scatter:
    def __init__(self, here, acc, slots, send, recv):
        self.here, self.acc, self.slots, self.send, self.recv = here, acc, slots, send, recv

    def index(self, j, o, stage, last):
        order = ORDERS[o]
        fixed = {order[k]: self.here.co[order[k]] for k in range(stage)}
        fixed[order[stage]] = last
        return (j,) + tuple(fixed.get(a, slice(None)) for a in range(3))

    def copies(self, j, o, stage):
        axis = ORDERS[o][stage]
        return [
            pltpu.make_async_remote_copy(
                src_ref=self.acc.at[self.index(j, o, stage, self.here.near[axis][i + 1])],
                dst_ref=self.slots[stage].at[j, i],
                send_sem=self.send.at[j, stage, i],
                recv_sem=self.recv.at[j, stage, i],
                device_id=self.here.peer(axis, i + 1),
            )
            for i in range(3)
        ]

    def step(self, k, j, o):
        if k > 0:
            for copy in self.copies(j, o, k - 1):
                copy.wait_recv()
            at = self.index(j, o, k - 1, self.here.co[ORDERS[o][k - 1]])
            got = self.slots[k - 1]
            self.acc[at] = (self.acc[at] + got[j, 0]) + (got[j, 1] + got[j, 2])
        if k < 3:
            for copy in self.copies(j, o, k):
                copy.start()

    def drain(self, j, o):
        for stage in range(3):
            for copy in self.copies(j, o, stage):
                copy.wait_send()


def scatter_scratch(tiles, dtype):
    dims = ((SIDE, SIDE), (SIDE,), ())
    slots = [pltpu.VMEM((tiles, 3, *d, 16, WIDE), dtype) for d in dims]
    sems = [pltpu.SemaphoreType.DMA((tiles, 3, 3))] * 2
    return [pltpu.VMEM((tiles, SIDE, SIDE, SIDE, 16, WIDE), dtype)] + slots + sems


class Spread:
    def __init__(self, here, lanes, buffer):
        self.here, self.lanes, self.buffer, self.flying = here, lanes, buffer, []
        self.width = buffer.shape[-1]

    def send(self, index, peer):
        return self.lanes.go(lambda: (self.buffer.at[index], self.buffer.at[index], peer()))

    def step(self, k):
        h, c = self.here, self.here.c
        for copy in self.flying:
            copy.wait_recv()
        every = slice(None)
        cut = self.width // WIDE // 2 * WIDE
        low, high = slice(0, cut), slice(cut, self.width)
        if k == 0:
            at = [((c, h.z, h.x, every, low), 2), ((c, h.z, h.x, every, high), 1)]
        elif k == 1:
            at = [((c, h.z, every, every, low), 1), ((c, every, h.x, every, high), 2)]
        else:
            at = []
        self.flying = [
            self.send(index, lambda axis=axis, s=s: h.peer(axis, s))
            for index, axis in at
            for s in (1, 3, 2)
        ]
        if k == 2:
            self.flying = [self.send((c,), lambda: h.peer(3, 1))]
        for copy in self.flying:
            copy.start()


class Gather:
    def __init__(self, here, lanes, block, shard, part):
        self.here, self.lanes, self.block, self.shard = here, lanes, block, shard
        y = here.y
        self.left, self.right, self.far = here.near[0][3], here.near[0][1], here.near[0][2]
        wide = 3 * WIDE
        lone = part - 2 * wide
        quarter, eighth, mid = shard // 4, shard // 8, shard // 2
        cuts = ((lone, 2), (lone + wide, 1))
        self.pieces, self.relays = [], []
        for column, axis in cuts:
            me = here.co[axis] * quarter
            self.pieces += self.pair(y, y, me, me, quarter, column, wide, 0)
            self.relays += self.pair(
                self.left, self.right, me, me + eighth, eighth, column, wide, 0
            )
        self.lone = self.pair(y, y, 0, 0, shard, 0, lone, 0)
        self.lone_relay = self.pair(self.left, self.right, 0, mid, mid, 0, lone, 0)
        self.around, self.passed = {}, {}
        for n, s in (("left", self.left), ("right", self.right), ("far", self.far)):
            self.around[n], self.passed[n] = [], []
            for column, axis in cuts:
                me = here.co[axis] * quarter
                down, up = here.near[axis][3] * quarter, here.near[axis][1] * quarter
                self.around[n] += self.pair(s, s, me, me, quarter, column, wide, axis)
                self.passed[n] += self.pair(s, s, down, up + eighth, eighth, column, wide, axis)

    def pair(self, s_up, s_down, at_up, at_down, count, column, size, axis):
        def trip(s, at, step):
            def ends():
                ref = lambda: self.block(s, at, count, column, size)
                return ref(), ref(), self.here.peer(axis, step)

            return self.lanes.go(ends)

        return [trip(s_up, at_up, 1), trip(s_down, at_down, 3)]


def start(copies):
    for copy in copies:
        copy.start()


def arrive(copies):
    for copy in copies:
        copy.wait_recv()


def forward_kernel(
    meta_ref, hidden_ref, gain_ref, cot_ref, table_ref,
    norm_out, cot_out, slope_out, slope_t_out, emb_ref, scale_out, loss_ref, meta_out,
    table, norm, tall, pre, slope, crecv, sbuf, meta, id_col, scale, mine, slot_r, slot_f,
    acc, slots0, slots1, slots2, tile_send, tile_recv,
    send_sem, recv_sem, core_send, core_recv, local_sem,
):
    here = Here()
    y, z, x, c = here.y, here.z, here.x, here.c
    rows, width = table_ref.shape
    part = width // 2
    shard = hidden_ref.shape[0]
    tokens = SIDE * shard
    tiles = part // WIDE
    padded = table.shape[1]
    first_row = (y * 32 + here.v) * rows
    lanes = Lanes(send_sem, recv_sem)
    scatter = Scatter(here, acc, (slots0, slots1, slots2), tile_send, tile_recv)

    loads = [
        pltpu.make_async_copy(
            table_ref.at[:, pl.ds(h * part, part)], table.at[h, pl.ds(0, rows)], local_sem.at[h]
        )
        for h in (0, 1)
    ]
    for load in loads:
        load.start()
    row, face = here.row(), here.face()
    row_at, face_at = x * 2 + c, y * SIDE + z
    here.enter(row, face)

    meta[y] = meta_ref[...]
    meta_copies = [
        lanes.go(lambda s=s: (meta_ref, meta.at[y], here.peer(0, s))) for s in (1, 2, 3)
    ]
    for copy in meta_copies:
        copy.start()

    own = of(y * shard, shard)

    def normalize(i, carry):
        at = pl.ds(of(i * 64, 64), 64)
        wide = hidden_ref[at, :].astype(F32)
        inv = lax.rsqrt(jnp.sum(wide * wide, axis=1, keepdims=True) / width + EPSILON)
        out = (wide * inv * gain_ref[...]).astype(BF16)
        to = pl.ds(of(own + i * 64, 64), 64)
        norm[0, to, :] = out[:, :part]
        norm[1, to, :] = out[:, part:]
        return carry

    lax.fori_loop(0, shard // 64, normalize, 0)

    def norm_block(s, offset, count, column, size):
        return norm.at[c, pl.ds(of(s * shard + offset, 16), count), pl.ds(column, size)]

    def cot_block(s, offset, count, column, size):
        at = pl.ds(of(s * shard + offset, 16), count)
        return cot_out.at[at, pl.ds(of(c * part + column, LANES), size)]

    normed = Gather(here, lanes, norm_block, shard, part)
    cots = Gather(here, lanes, cot_block, shard, part)
    across = {
        n: lanes.go(
            lambda s=s: (
                norm_block(s, 0, shard, 0, part), norm_block(s, 0, shard, 0, part), here.peer(3, 1)
            )
        )
        for n, s in (("left", normed.left), ("right", normed.right), ("far", normed.far))
    }
    start(normed.pieces)
    cot_local = pltpu.make_async_copy(cot_ref, cot_out.at[pl.ds(own, shard), :], local_sem.at[2])
    cot_local.start()

    for copy in meta_copies:
        copy.wait_recv()
    for s in range(SIDE):
        local = (meta[s, 0:1, :] - first_row).astype(F32)
        id_col[s * shard : (s + 1) * shard, :] = jnp.transpose(
            jnp.broadcast_to(local, (LANES, shard))
        ).astype(I32)

    def onehot(i, carry):
        at = pl.ds(of(i * 64, 64), 64)
        ids = id_col[at, :]
        lane = lax.broadcasted_iota(I32, (64, LANES), 1)
        for t in range(padded // LANES):
            inside = lane + t * LANES
            hit = ids == (jnp.where(inside < rows, inside, -1) if (t + 1) * LANES > rows else inside)
            tall[at, t * LANES : (t + 1) * LANES] = jnp.where(hit, 1.0, 0.0).astype(BF16)
        return carry

    lax.fori_loop(0, tokens // 64, onehot, 0)
    for h in (0, 1):
        table[h, rows:padded, :] = jnp.zeros((padded - rows, part), BF16)
    for load in loads:
        load.wait()

    def core_copy(j):
        return pltpu.make_async_remote_copy(
            src_ref=sbuf.at[odd(j)],
            dst_ref=crecv.at[j],
            send_sem=core_send.at[j],
            recv_sem=core_recv.at[j],
            device_id=here.peer(3, 1),
        )

    blocks = (SIDE, SIDE, SIDE, 16, WIDE)

    def find(j, carry):
        columns = pl.ds(of(j * WIDE, WIDE), WIDE)

        def product(h):
            out = jnp.dot(tall[...], table[h, :, columns], preferred_element_type=F32)
            return out.astype(BF16).reshape(blocks)

        @pl.when(j >= 2)
        def _():
            core_copy(j - 2).wait_send()

        other, mine_tile = product(1 - c), product(c)
        sbuf[odd(j)] = other
        acc[j] = mine_tile
        core_copy(j).start()

        @pl.when(j == 1)
        def _():
            arrive(normed.pieces)
            start(normed.relays + normed.around["left"] + normed.around["right"] + normed.lone)

        @pl.when(j == 3)
        def _():
            arrive(normed.relays)
            start(normed.around["far"])

        @pl.when(j == 4)
        def _():
            arrive(normed.around["left"] + normed.around["right"])
            start(normed.passed["left"] + normed.passed["right"])
            arrive(normed.lone)
            start(normed.lone_relay)

        @pl.when(j == 5)
        def _():
            arrive(normed.around["far"])
            start(normed.passed["far"])
            cot_local.wait()
            start(cots.pieces)

        @pl.when(j == 6)
        def _():
            arrive(normed.passed["left"] + normed.passed["right"])
            start([across["left"], across["right"]])

        return carry

    lax.fori_loop(0, tiles, find, 0)
    arrive(normed.lone_relay + normed.passed["far"])
    across["far"].start()
    for j in range(tiles):
        core_copy(j).wait_recv()
        acc[j] = acc[j] + crecv[j]
        scatter.step(0, j, j % 3)
    arrive(list(across.values()))
    norm_copies = [
        pltpu.make_async_copy(norm.at[h], norm_out.at[h], local_sem.at[3 + h]) for h in (0, 1)
    ]
    for copy in norm_copies:
        copy.start()

    group = 2 * shard
    tall_rows = rows // 5
    def target_of(g):
        both_rows = [meta[2 * g + i, 1:2, :] - first_row for i in (0, 1)]
        row = jnp.concatenate(both_rows, axis=1)
        return jnp.where((row >= 0) & (row < rows), row, -1)

    def weight_of(g):
        return jnp.concatenate([meta[2 * g + i, 2:3, :] for i in (0, 1)], axis=1).astype(F32)

    def found_step(k):
        for j in range(tiles):
            scatter.step(k, j, j % 3)

    def emit():
        for j in range(tiles):
            found = acc[j, y, z, x].astype(F32) * math.sqrt(width)
            emb_ref[:, j * WIDE : (j + 1) * WIDE] = found.astype(BF16)

    def cot_start():
        arrive(cots.pieces)
        start(cots.relays + cots.around["left"] + cots.around["right"] + cots.lone)

    def cot_far():
        arrive(cots.relays)
        start(cots.around["far"])

    def cot_pass():
        arrive(cots.around["left"] + cots.around["right"] + cots.lone)
        start(cots.passed["left"] + cots.passed["right"] + cots.lone_relay)

    def cot_last():
        arrive(cots.around["far"])
        start(cots.passed["far"])

    plan = {0: cot_start, 2: cot_far, 4: cot_pass, 5: lambda: found_step(1), 6: cot_last,
            7: lambda: found_step(2)}

    def exchange_start(g, stage):
        me, slots = ((row_at, slot_r), (face_at, slot_f))[stage]
        peers = (row, face)[stage]
        slots[g, me] = mine[g, stage]
        out = [
            lanes.go(lambda p=p: (mine.at[g, stage], slots.at[g, me], p)) for p in peers
        ]
        start(out)
        return out

    def exchange_step(g, stage, flying):
        arrive(flying)
        slots = (slot_r, slot_f)[stage - 1]
        parts = [slots[g, i] for i in range(slots.shape[1])]
        while len(parts) > 1:
            parts = [a + b for a, b in zip(parts[::2], parts[1::2])]
        mine[g, stage] = parts[0]
        return exchange_start(g, stage) if stage < 2 else []

    flights = {}
    for g in (0, 1):
        target = target_of(g)
        token_at = slice(g * group, (g + 1) * group)

        def logits(r, carry, g=g, target=target, token_at=token_at):
            at = pl.ds(of(r * tall_rows, 16), tall_rows)
            raw = [
                lax.dot_general(
                    table[h, at, :], norm[h, token_at, :],
                    (((1,), (1,)), ((), ())), preferred_element_type=F32,
                )
                for h in (0, 1)
            ]
            pre[at, token_at] = raw[0] + raw[1]

            def shape(i, sums):
                total, picked = sums
                rows_at = pl.ds(of(r * tall_rows + i * 40, 8), 40)
                bent = jnp.tanh(pre[rows_at, token_at] * (1.0 / SOFTCAP))
                grown = jnp.exp(bent * SOFTCAP)
                pre[rows_at, token_at] = grown * (1.0 - bent * bent)
                ids = lax.broadcasted_iota(I32, bent.shape, 0) + (r * tall_rows + i * 40)
                found = jnp.where(ids == target, bent, 0.0)
                fold = lambda a: jnp.sum(a.reshape(5, 8, group), axis=0)
                return total + fold(grown), picked + fold(found)

            carry = lax.fori_loop(0, tall_rows // 40, shape, carry)
            for i in range(5):
                k = 5 * g + i
                if k in plan:

                    @pl.when(r == i)
                    def _(k=k):
                        plan[k]()

            if g == 1:
                for i in (1, 2):

                    @pl.when(r == 2 * i - 1)
                    def _(i=i):
                        flights[0] = exchange_step(0, i, flights[0])

            return carry

        zero = jnp.zeros((8, group), F32)
        total, picked = lax.fori_loop(0, 5, logits, (zero, zero))
        total = jnp.sum(total, axis=0, keepdims=True)
        picked = jnp.sum(picked, axis=0, keepdims=True)
        for i in range(group // LANES):
            mine[g, 0, i : i + 1, :] = total[:, i * LANES : (i + 1) * LANES]
            mine[g, 0, 4 + i : 5 + i, :] = picked[:, i * LANES : (i + 1) * LANES]
        flights[g] = exchange_start(g, 0)

    pre[rows:padded, :] = jnp.zeros((padded - rows, tokens), F32)
    sums = []

    def slopes(g):
        target, weight = target_of(g), weight_of(g)
        stats = mine[g, 2]
        lines = [jnp.concatenate([stats[i + 4 * k : i + 4 * k + 1] for i in range(4)], axis=1) for k in (0, 1)]
        total, bent = lines
        chosen = jnp.exp(bent * SOFTCAP) / total
        sums.append(
            (
                jnp.sum(weight * (jnp.log(total) - SOFTCAP * bent), axis=1, keepdims=True),
                jnp.sum(weight, axis=1, keepdims=True),
            )
        )
        bound = 0.17 * (jnp.maximum(1.0 - chosen, 0.0) + 1e-5)
        scale[g * group : (g + 1) * group, :] = jnp.transpose(
            jnp.broadcast_to(bound, (LANES, group))
        )
        factor = weight / total
        drop = weight * (1.0 - bent * bent)

        def turn(i, carry):
            at = pl.ds(of(i * WIDE, WIDE), WIDE)
            ids = lax.broadcasted_iota(I32, (WIDE, shard), 0) + i * WIDE
            for s in (0, 1):
                here_at = slice(g * group + s * shard, g * group + (s + 1) * shard)
                cut = slice(s * shard, (s + 1) * shard)
                value = pre[at, here_at] * factor[:, cut]
                value = value - jnp.where(ids == target[:, cut], drop[:, cut], 0.0)
                low = value.astype(BF16)
                slope[at, here_at] = low
                tall[here_at, at] = jnp.transpose(low)
            return carry

        lax.fori_loop(0, padded // WIDE, turn, 0)
        copies = []
        for k, (src, dst) in enumerate(
            ((slope.at[:, g * group : (g + 1) * group], slope_out.at[:, g * group : (g + 1) * group]),
             (tall.at[g * group : (g + 1) * group], slope_t_out.at[g * group : (g + 1) * group]))
        ):
            copies.append(pltpu.make_async_copy(src, dst, local_sem.at[5 + 2 * g + k]))
            copies[-1].start()
        return copies

    found_step(3)
    emit()
    flights[1] = exchange_step(1, 1, flights[1])
    out_copies = slopes(0)
    flights[1] = exchange_step(1, 2, flights[1])
    out_copies += slopes(1)
    loss = (sums[0][0] + sums[1][0]) / jnp.maximum(sums[0][1] + sums[1][1], 1.0)
    loss_ref[...] = jnp.broadcast_to(loss, loss_ref.shape)
    meta_out[...] = meta[...]
    scale_copy = pltpu.make_async_copy(scale, scale_out, local_sem.at[9])
    scale_copy.start()
    arrive(cots.passed["left"] + cots.passed["right"] + cots.passed["far"] + cots.lone_relay)
    for copy in out_copies + [scale_copy] + norm_copies:
        copy.wait()
    for copy in lanes.made:
        if copy.gone:
            copy.wait_send()
    for j in range(tiles):
        if j >= tiles - 2:
            core_copy(j).wait_send()
        scatter.drain(j, j % 3)


def backward_kernel(
    slope_t_ref, scale_ref, ids_ref, emb_ref, hidden_ref, gain_ref, slope_ref, norm_ref, cot_ref, table_ref,
    grad_out, emb_out, gain_out, head_out, cot_other,
    table, norm, slope, hit, crecv, sbuf, held, grad, emb, cots, wide, up, dots, gains, slot_g, slot_c,
    acc, slots0, slots1, slots2, tile_send, tile_recv,
    send_sem, recv_sem, core_send, core_recv, local_sem, cot_sem, out_sem,
):
    here = Here()
    y, z, x, c = here.y, here.z, here.x, here.c
    rows, width = table_ref.shape
    part = width // 2
    tiles = part // WIDE
    padded = table.shape[1]
    tokens = slope_t_ref.shape[0]
    shard = tokens // SIDE
    lanes = Lanes(send_sem, recv_sem)
    scatter = Scatter(here, acc, (slots0, slots1, slots2), tile_send, tile_recv)
    blocks = (SIDE, SIDE, SIDE, 16, WIDE)
    first_row = (y * 32 + here.v) * rows

    def load(h):
        return pltpu.make_async_copy(
            table_ref.at[:, pl.ds(of(h * part, LANES), part)],
            table.at[h, pl.ds(0, rows)],
            local_sem.at[4 + h],
        )

    load(1 - c).start()
    load(c).start()
    mine_at = (z * SIDE + x) * 16
    row_loads = [
        pltpu.make_async_copy(
            hidden_ref.at[pl.ds(of(mine_at, 16), 16), pl.ds(h * part, part)],
            wide.at[h],
            local_sem.at[h],
        )
        for h in (0, 1)
    ]
    later = [
        pltpu.make_async_copy(slope_ref, slope, local_sem.at[6]),
        pltpu.make_async_copy(norm_ref, norm, local_sem.at[7]),
    ]
    for copy in row_loads + later:
        copy.start()
    here.enter(here.axes(), [here.peer(3, 1)])
    cot_across = lanes.go(
        lambda: (
            cot_ref.at[:, pl.ds(of(c * part, LANES), part)], cot_other, here.peer(3, 1)
        )
    )
    emb[c, z, x] = emb_ref[...]
    emb_spread, spread = Spread(here, lanes, emb), Spread(here, lanes, grad)
    emb_spread.step(0)
    for h in (0, 1):
        table[h, rows:padded, :] = jnp.zeros((padded - rows, part), BF16)

    def match(i, carry):
        at = pl.ds(of(i * 80, 16), 80)
        ids = lax.broadcasted_iota(I32, (80, shard), 0) + (first_row + i * 80)
        for s in range(SIDE):
            found = jnp.where(ids == ids_ref[s, 0:1, :], 1.0, 0.0)
            hit[at, s * shard : (s + 1) * shard] = found.astype(BF16)
        return carry

    lax.fori_loop(0, rows // 80, match, 0)

    def core_copy(j):
        return pltpu.make_async_remote_copy(
            src_ref=sbuf.at[odd(j)],
            dst_ref=crecv.at[j],
            send_sem=core_send.at[j],
            recv_sem=core_recv.at[j],
            device_id=here.peer(3, 1),
        )

    delays = (1, 5, 7, 9)

    def substeps(s):
        for k in range(4):
            j = s - delays[k]

            @pl.when((j >= 0) & (j < tiles))
            def _(k=k, j=j):
                if k == 0:
                    core_copy(j).wait_recv()

                    def fit(i, carry):
                        at = pl.ds(of(i * shard, shard), shard)
                        factor = FULL / scale_ref[at, :]
                        total = held[odd(j), at, :] + crecv[j, at, :]
                        total = total * jnp.concatenate([factor] * (WIDE // LANES), axis=1)
                        whole = jnp.round(total).astype(I32).astype(I16)
                        acc[j, i] = whole.reshape(blocks[1:])
                        return carry

                    lax.fori_loop(0, SIDE, fit, 0)
                for o in range(3):

                    @pl.when(lax.rem(j, 3) == o)
                    def _(o=o):
                        scatter.step(k, j, o)

    def tile(j, carry):
        columns = pl.ds(of(j * WIDE, WIDE), WIDE)

        def product(h):
            return jnp.dot(slope_t_ref[...], table[h, :, columns], preferred_element_type=F32)

        @pl.when(j >= 2)
        def _():
            core_copy(j - 2).wait_send()

        other, mine_tile = product(1 - c), product(c)
        sbuf[odd(j)] = other
        held[odd(j)] = mine_tile
        core_copy(j).start()
        substeps(j)
        for i, k in ((2, 1), (5, 2)):

            @pl.when(j == i)
            def _(k=k):
                emb_spread.step(k)

        return carry

    load(1 - c).wait()
    load(c).wait()
    lax.fori_loop(0, tiles, tile, 0)
    cot_across.start()
    for copy in row_loads + later:
        copy.wait()

    def cot_loads(g):
        j = lax.rem(g, tiles)
        mine_half = cot_ref.at[:, pl.ds(of(c * part + j * WIDE, LANES), WIDE)]
        other_half = cot_other.at[:, pl.ds(of(j * WIDE, LANES), WIDE)]
        return [
            pltpu.make_async_copy(half, cots.at[odd(g)], cot_sem.at[odd(g)])
            for half in (mine_half, other_half)
        ]

    def cot_start(g):
        @pl.when(g < tiles)
        def _():
            cot_loads(g)[0].start()

        @pl.when(g >= tiles)
        def _():
            cot_loads(g)[1].start()

    def head_copy(g):
        j = lax.rem(g, tiles)
        h = jnp.where(g < tiles, c, 1 - c)
        return pltpu.make_async_copy(
            table.at[h, pl.ds(0, rows), pl.ds(of(j * WIDE, WIDE), WIDE)],
            head_out.at[:, pl.ds(of(h * part + j * WIDE, LANES), WIDE)],
            out_sem.at[g],
        )

    flying = {}

    def gain_send(stage):
        axis = (2, 1, 0)[stage]
        slot_g[stage, here.co[axis]] = gains[stage]
        out = [
            lanes.go(
                lambda s=s: (gains.at[stage], slot_g.at[stage, here.co[axis]], here.peer(axis, s))
            )
            for s in (1, 2, 3)
        ]
        start(out)
        flying["gain"] = out

    def gain_sum(stage):
        arrive(flying["gain"])
        slots = [slot_g[stage, i] for i in range(SIDE)]
        gains[stage + 1] = (slots[0] + slots[1]) + (slots[2] + slots[3])

    def pieces():
        both = [wide[h].astype(F32) for h in (0, 1)]
        square = sum(jnp.sum(b * b, axis=1, keepdims=True) for b in both) / width
        return lax.rsqrt(square + EPSILON), wide[c].astype(F32)

    def finish():
        unit = scale_ref[pl.ds(of(y * shard + mine_at, 16), 16), 0:1] * (1.0 / FULL)
        for j in range(tiles):
            up[:, j * WIDE : (j + 1) * WIDE] = acc[j, y, z, x].astype(I32).astype(F32) * unit
        inv, ours = pieces()
        dot = jnp.sum(up[...] * gain_ref[c] * ours, axis=1, keepdims=True)
        dots[0] = jnp.broadcast_to(dot, (16, LANES))
        slot_c[c] = dots[0]
        flying["dot"] = [lanes.go(lambda: (dots.at[0], slot_c.at[c], here.peer(3, 1)))]
        start(flying["dot"])
        gain_part = jnp.sum(up[...] * ours * inv, axis=0, keepdims=True)
        for j in range(part // LANES):
            gains[0, j : j + 1, :] = gain_part[:, j * LANES : (j + 1) * LANES]
        lines = gains.shape[1]
        gains[0, part // LANES : lines, :] = jnp.zeros((lines - part // LANES, LANES), F32)
        gain_send(0)

    def gradient():
        arrive(flying["dot"])
        inv, ours = pieces()
        mean_dot = (slot_c[0, :, 0:1] + slot_c[1, :, 0:1]) / width
        out = inv * (up[...] * gain_ref[c]) - ours * (inv * inv * inv) * mean_dot
        grad[c, z, x] = out.astype(BF16)
        spread.step(0)

    def gain_last():
        gain_sum(2)
        gain_out[c] = gains[3]
        slot_g[3, c] = gains[3]
        flying["gain"] = [lanes.go(lambda: (gains.at[3], slot_g.at[3, c], here.peer(3, 1)))]
        start(flying["gain"])

    def wide_out(buffer, out, at):
        return [
            pltpu.make_async_copy(
                buffer.at[h], out.at[:, :, :, pl.ds(h * part, part)], local_sem.at[at + h]
            )
            for h in (0, 1)
        ]

    plan = {
        3: lambda: (arrive(emb_spread.flying), [o.start() for o in wide_out(emb, emb_out, 2)]),
        5: lambda: arrive([cot_across]),
        8: finish,
        9: lambda: (gradient(), gain_sum(0), gain_send(1)),
        11: lambda: (spread.step(1), gain_sum(1), gain_send(2)),
        13: lambda: (spread.step(2), gain_last()),
    }
    cot_start(0)

    def head(g, carry):
        j = lax.rem(g, tiles)
        h = jnp.where(g < tiles, c, 1 - c)
        columns = pl.ds(of(j * WIDE, WIDE), WIDE)

        @pl.when(g + 1 < 2 * tiles)
        def _():
            cot_start(g + 1)

        cot_loads(g)[0].wait()
        first = jnp.dot(slope[0:rows, :], norm[h, :, columns], preferred_element_type=F32)
        second = jnp.dot(hit[...], cots[odd(g)], preferred_element_type=F32)
        table[h, 0:rows, columns] = (first + second * math.sqrt(width)).astype(BF16)
        head_copy(g).start()
        substeps(g + tiles)
        for i in plan:

            @pl.when(g == i)
            def _(i=i):
                plan[i]()

        return carry

    lax.fori_loop(0, 2 * tiles, head, 0)
    arrive(spread.flying)
    outs = wide_out(grad, grad_out, 0)
    for copy in outs:
        copy.start()
    arrive(flying["gain"])
    gain_out[1 - c] = slot_g[3, 1 - c]
    for copy in outs + wide_out(emb, emb_out, 2):
        copy.wait()

    def heads_done(g, carry):
        head_copy(g).wait()
        return carry

    lax.fori_loop(0, 2 * tiles, heads_done, 0)
    for copy in lanes.made:
        if copy.gone:
            copy.wait_send()
    for j in range(tiles):
        if j >= tiles - 2:
            core_copy(j).wait_send()
        scatter.drain(j, j % 3)


def body(input_ids, target_ids, loss_mask, final_hidden, norm_gain, embed_cotangent, table):
    rows, width = table.shape
    shard = final_hidden.shape[0]
    tokens, part = SIDE * shard, width // 2
    tiles = part // WIDE
    padded = -(-rows // WIDE) * WIDE
    group = 2 * shard
    first_row = lax.axis_index(("dp", "vocab")) * rows
    meta = jnp.pad(jnp.stack([input_ids, target_ids, loss_mask]), ((0, 5), (0, 0)))
    any_ = pl.BlockSpec(memory_space=pl.ANY)
    vmem = pl.BlockSpec(memory_space=pltpu.VMEM)
    dma = pltpu.SemaphoreType.DMA
    share = (SIDE, SIDE, 16)
    blocks = (SIDE, SIDE, SIDE, 16, WIDE)
    norm_all, cot_all, slope, slope_t, found, bound, loss, meta_all = pl.pallas_call(
        forward_kernel,
        out_shape=(
            jax.ShapeDtypeStruct((2, tokens, part), BF16),
            jax.ShapeDtypeStruct((tokens, width), BF16),
            jax.ShapeDtypeStruct((padded, tokens), BF16),
            jax.ShapeDtypeStruct((tokens, padded), BF16),
            jax.ShapeDtypeStruct((16, part), BF16),
            jax.ShapeDtypeStruct((tokens, LANES), F32),
            jax.ShapeDtypeStruct((8, LANES), F32),
            jax.ShapeDtypeStruct((SIDE, 8, shard), I32),
        ),
        in_specs=[vmem, vmem, vmem, vmem, any_],
        out_specs=(any_, any_, any_, any_, vmem, any_, vmem, vmem),
        scratch_shapes=[
            pltpu.VMEM((2, padded, part), BF16),
            pltpu.VMEM((2, tokens, part), BF16),
            pltpu.VMEM((tokens, padded), BF16),
            pltpu.VMEM((padded, tokens), F32),
            pltpu.VMEM((padded, tokens), BF16),
            pltpu.VMEM((tiles, *blocks), BF16),
            pltpu.VMEM((2, *blocks), BF16),
            pltpu.VMEM((SIDE, 8, shard), I32),
            pltpu.VMEM((tokens, LANES), I32),
            pltpu.VMEM((tokens, LANES), F32),
            pltpu.VMEM((2, 3, 8, LANES), F32),
            pltpu.VMEM((2, 8, 8, LANES), F32),
            pltpu.VMEM((2, 16, 8, LANES), F32),
            *scatter_scratch(tiles, BF16),
            dma((140,)), dma((140,)), dma((tiles,)), dma((tiles,)), dma((12,)),
        ],
        compiler_params=pltpu.CompilerParams(
            collective_id=1, has_side_effects=True, vmem_limit_bytes=62 * 1024 * 1024
        ),
    )(meta, final_hidden, norm_gain.reshape(1, width), embed_cotangent, table)
    grad, embedded, gain, head, _ = pl.pallas_call(
        backward_kernel,
        out_shape=(
            jax.ShapeDtypeStruct((*share, width), BF16),
            jax.ShapeDtypeStruct((*share, width), BF16),
            jax.ShapeDtypeStruct((2, 16, LANES), F32),
            jax.ShapeDtypeStruct((rows, width), BF16),
            jax.ShapeDtypeStruct((tokens, part), BF16),
        ),
        in_specs=[vmem, vmem, vmem, vmem, any_, vmem, any_, any_, any_, any_],
        out_specs=(any_, any_, vmem, any_, any_),
        scratch_shapes=[
            pltpu.VMEM((2, padded, part), BF16),
            pltpu.VMEM((2, tokens, part), BF16),
            pltpu.VMEM((padded, tokens), BF16),
            pltpu.VMEM((rows, tokens), BF16),
            pltpu.VMEM((tiles, tokens, WIDE), F32),
            pltpu.VMEM((2, tokens, WIDE), F32),
            pltpu.VMEM((2, tokens, WIDE), F32),
            pltpu.VMEM((2, *share, part), BF16),
            pltpu.VMEM((2, *share, part), BF16),
            pltpu.VMEM((2, tokens, WIDE), BF16),
            pltpu.VMEM((2, 16, part), BF16),
            pltpu.VMEM((16, part), F32),
            pltpu.VMEM((1, 16, LANES), F32),
            pltpu.VMEM((4, 16, LANES), F32),
            pltpu.VMEM((4, SIDE, 16, LANES), F32),
            pltpu.VMEM((2, 16, LANES), F32),
            *scatter_scratch(tiles, I16),
            dma((50,)), dma((50,)), dma((tiles,)), dma((tiles,)), dma((8,)), dma((2,)),
            dma((2 * tiles,)),
        ],
        compiler_params=pltpu.CompilerParams(
            collective_id=2, has_side_effects=True, vmem_limit_bytes=63 * 1024 * 1024
        ),
    )(
        slope_t, bound, meta_all, found, final_hidden, norm_gain.reshape(2, 1, part),
        slope, norm_all, cot_all, table,
    )
    gain_grad = gain[:, : part // LANES, :].reshape(width)
    return (
        embedded.reshape(shard, width),
        loss[0, 0],
        grad.reshape(shard, width),
        gain_grad,
        head,
    )


def solution(mesh):
    placed = (
        P("dp"),
        P("dp"),
        P("dp"),
        P("dp", None),
        P(),
        P("dp", None),
        P(("dp", "vocab"), None),
    )
    return jax.shard_map(
        body,
        mesh=mesh,
        in_specs=placed,
        out_specs=(P("dp", None), P(), P("dp", None), P(), P(("dp", "vocab"), None)),
        check_vma=False,
    )
```

```python
import functools
import math

import jax
import jax.numpy as jnp
from jax import lax
from jax.experimental import pallas as pl
from jax.experimental.pallas import tpu as pltpu
from jax.sharding import PartitionSpec as P

SOFTCAP = 30
EPSILON = 1e-06
LANES = 128
F32, BF16, I16, I32 = jnp.float32, jnp.bfloat16, jnp.int16, jnp.int32

VMEM_BYTES = 67043328
SIDE = 4
BLOCKS = 25
WIDE = 256
FULL = 32000.0
LATE = 1
MOVES = {
    "f1": (0, 7), "f2": (0, 9), "f3": (1, 1), "g1": (1, 4), "g2": (1, 6), "g3": (2, 1),
    "e0": (2, 2), "e1": (2, 5), "e2": (3, 0),
    "c0": (0, 9), "c1": (1, 2), "c2": (1, 4), "c3": (1, 6), "c4": (2, 2), "c5": (2, 5),
}
DELAYS = (1, 4, 6, 8)
ORDERS = ((0, 2, 1), (2, 1, 0), (1, 0, 2))
FIRST = (0, 2, 1)


def of(value, step):
    return value if isinstance(value, int) else pl.multiple_of(value, step)


def third(j):
    return j % 3 if isinstance(j, int) else lax.rem(j, 3)


def odd(j):
    return j % 2 if isinstance(j, int) else lax.rem(j, 2)


class Here:
    def __init__(self):
        self.y = lax.axis_index("dp")
        self.v = lax.axis_index("vocab")
        self.z = lax.div(self.v, 8)
        self.x = lax.rem(lax.div(self.v, 2), SIDE)
        self.c = lax.rem(self.v, 2)
        self.co = (self.y, self.z, self.x)
        self.near = [[p] + [lax.rem(p + s, SIDE) for s in (1, 2, 3)] for p in self.co]

    def peer(self, axis, step):
        if axis == 0:
            return {"dp": lax.rem(self.y + step, SIDE)}
        if axis == 1:
            return {"vocab": lax.rem(self.z + step, SIDE) * 8 + lax.rem(self.v, 8)}
        if axis == 2:
            return {"vocab": self.z * 8 + lax.rem(self.x + step, SIDE) * 2 + self.c}
        return {"vocab": self.v + 1 - 2 * self.c}

    def plus(self, axis, step):
        return self.near[axis][step]

    def enter(self, *groups):
        barrier = pltpu.get_barrier_semaphore()
        peers = [peer for group in groups for peer in group]
        for peer in peers:
            pl.semaphore_signal(barrier, inc=1, device_id=peer)
        return lambda: pl.semaphore_wait(barrier, len(peers))

    def offset(self, steps):
        z = self.near[1][steps.get(1, 0)]
        x = self.near[2][steps.get(2, 0)]
        return {"dp": self.near[0][steps.get(0, 0)], "vocab": z * 8 + x * 2 + self.c}

    def row(self):
        out = []
        for i in range(1, 8):
            x = self.near[2][i // 2]
            out.append({"vocab": self.z * 8 + x * 2 + (1 - self.c if i % 2 else self.c)})
        return out

    def face(self, first, second):
        return [self.offset({first: i // 4, second: i % 4}) for i in range(1, 16)]

    def all_faces(self):
        near = [self.offset({a: s}) for a in range(3) for s in (1, 2, 3)]
        pairs = ((0, 1), (0, 2), (1, 2))
        far = [
            self.offset({a: i, b: k}) for a, b in pairs for i in (1, 2, 3) for k in (1, 2, 3)
        ]
        return near + far + [self.peer(3, 1)]


class Lanes:
    def __init__(self, send, recv):
        self.send, self.recv, self.made = send, recv, []

    def go(self, ends):
        self.made.append(Trip(self, len(self.made), ends))
        return self.made[-1]


class Trip:
    def __init__(self, lanes, i, ends):
        self.lanes, self.i, self.ends, self.gone = lanes, i, ends, False

    def make(self):
        src, dst, device = self.ends()
        return pltpu.make_async_remote_copy(
            src_ref=src,
            dst_ref=dst,
            send_sem=self.lanes.send.at[self.i],
            recv_sem=self.lanes.recv.at[self.i],
            device_id=device,
        )

    def start(self):
        self.gone = True
        self.make().start()

    def wait_recv(self):
        self.make().wait_recv()

    def wait_send(self):
        self.make().wait_send()


class Reduce:
    def __init__(self, here, acc, slots, grid, wide, send, recv):
        self.here, self.acc, self.slots, self.grid, self.wide = here, acc, slots, grid, wide
        self.send, self.recv = send, recv

    def at(self, j, where):
        return (j,) + tuple(where.get(a, slice(None)) for a in range(3))

    def own(self, j):
        return self.at(j, dict(enumerate(self.here.co)))

    def trip(self, j, n, src, dst, device):
        return pltpu.make_async_remote_copy(
            src_ref=src,
            dst_ref=dst,
            send_sem=self.send.at[j, n],
            recv_sem=self.recv.at[j, n],
            device_id=device,
        )

    def copies(self, j, o, part):
        here, axis = self.here, FIRST[o]
        if part == 0:
            return [
                self.trip(
                    j, i, self.acc.at[self.at(j, {axis: here.near[axis][i + 1]})],
                    self.slots.at[j, i], here.offset({axis: i + 1}),
                )
                for i in (0, 2, 1)
            ]
        if part == 1:
            a, b = [k for k in range(3) if k != axis]
            out = []
            for i in range(1, 16):
                where = {axis: here.co[axis], a: here.near[a][i // 4], b: here.near[b][i % 4]}
                out.append(
                    self.trip(
                        j, 2 + i, self.acc.at[self.at(j, where)], self.grid.at[j, i],
                        here.offset({a: i // 4, b: i % 4}),
                    )
                )
            return out
        if part == 2:
            mine = self.wide.at[here.c, j, here.z, here.x]
            return [
                self.trip(j, 17 + i, mine, mine, here.offset({1: i // 4, 2: i % 4}))
                for i in range(1, 16)
            ]
        whole = self.wide.at[here.c, j]
        return [self.trip(j, 33, whole, whole, here.peer(3, 1))]

    def step(self, k, j, o, last=None):
        if k > 0:
            arrive(self.copies(j, o, k - 1))
        if k == 1:
            at = self.at(j, {FIRST[o]: self.here.co[FIRST[o]]})
            got = [self.slots[j, i] for i in range(3)]
            self.acc[at] = (self.acc[at] + got[0]) + (got[1] + got[2])
        if k == 2:
            parts = [self.acc[self.own(j)]] + [self.grid[j, i] for i in range(1, 16)]
            while len(parts) > 1:
                parts = [a + b for a, b in zip(parts[::2], parts[1::2])]
            total = parts[0] if last is None else last(parts[0])
            self.wide[self.here.c, j, self.here.z, self.here.x] = total
        if k < 4:
            start(self.copies(j, o, k))

    def drain(self, j, o):
        for part in range(4):
            for copy in self.copies(j, o, part):
                copy.wait_send()


def reduce_scratch(tiles, dtype):
    sems = [pltpu.SemaphoreType.DMA((tiles, 34))] * 2
    return [
        pltpu.VMEM((tiles, SIDE, SIDE, SIDE, 16, WIDE), dtype),
        pltpu.VMEM((tiles, 3, SIDE, SIDE, 16, WIDE), dtype),
        pltpu.VMEM((tiles, 16, 16, WIDE), dtype),
        pltpu.VMEM((2, tiles, SIDE, SIDE, 16, WIDE), dtype),
        *sems,
    ]


class Scatter:
    def __init__(self, here, acc, slots, send, recv):
        self.here, self.acc, self.slots, self.send, self.recv = here, acc, slots, send, recv

    def index(self, j, order, stage, last, half):
        fixed = {order[k]: self.here.co[order[k]] for k in range(stage)}
        fixed[order[stage]] = last
        columns = slice(half * LANES, (half + 1) * LANES)
        return (j,) + tuple(fixed.get(a, slice(None)) for a in range(3)) + (slice(None), columns)

    def slot(self, j, i, stage, half):
        columns = slice(half * LANES, (half + 1) * LANES)
        return (j, i) + (slice(None),) * (3 - stage) + (columns,)

    def copies(self, j, o, stage):
        out = []
        for half in (0, 1):
            order = ORDERS[(o + half) % 3]
            axis = order[stage]
            for i in (0, 2, 1):
                out.append(
                    pltpu.make_async_remote_copy(
                        src_ref=self.acc.at[
                            self.index(j, order, stage, self.here.near[axis][i + 1], half)
                        ],
                        dst_ref=self.slots[stage].at[self.slot(j, i, stage, half)],
                        send_sem=self.send.at[j, stage, half, i],
                        recv_sem=self.recv.at[j, stage, half, i],
                        device_id=self.here.peer(axis, i + 1),
                    )
                )
        return out

    def step(self, k, j, o):
        if k > 0:
            for copy in self.copies(j, o, k - 1):
                copy.wait_recv()
            for half in (0, 1):
                order = ORDERS[(o + half) % 3]
                at = self.index(j, order, k - 1, self.here.co[order[k - 1]], half)
                got = [self.slots[k - 1][self.slot(j, i, k - 1, half)] for i in range(3)]
                self.acc[at] = (self.acc[at] + got[0]) + (got[1] + got[2])
        if k < 3:
            for copy in self.copies(j, o, k):
                copy.start()

    def drain(self, j, o):
        for stage in range(3):
            for copy in self.copies(j, o, stage):
                copy.wait_send()


def scatter_scratch(tiles, dtype):
    dims = ((SIDE, SIDE), (SIDE,), ())
    slots = [pltpu.VMEM((tiles, 3, *d, 16, WIDE), dtype) for d in dims]
    sems = [pltpu.SemaphoreType.DMA((tiles, 3, 2, 3))] * 2
    return [pltpu.VMEM((tiles, SIDE, SIDE, SIDE, 16, WIDE), dtype)] + slots + sems


class Spread:
    def __init__(self, here, lanes, buffer):
        self.here, self.lanes, self.buffer, self.flying = here, lanes, buffer, []
        self.part = buffer.shape[-1] // 2

    def at(self, z, x, column, size):
        start_at = of(self.here.c * self.part + column, LANES)
        return self.buffer.at[z, x, :, pl.ds(start_at, size)]

    def send(self, z, x, column, size, peer):
        def ends():
            return self.at(z, x, column, size), self.at(z, x, column, size), peer()

        return self.lanes.go(ends)

    def step(self, k):
        h = self.here
        arrive(self.flying)
        every = slice(None)
        cut = self.part // WIDE // 2 * WIDE
        rest = self.part - cut
        if k == 0:
            at = [((h.z, h.x, 0, cut), 2), ((h.z, h.x, cut, rest), 1)]
        elif k == 1:
            at = [((h.z, every, 0, cut), 1), ((every, h.x, cut, rest), 2)]
        else:
            at = []
        self.flying = [
            self.send(*where, lambda axis=axis, s=s: h.peer(axis, s))
            for where, axis in at
            for s in (1, 3, 2)
        ]
        if k == 2:
            self.flying = [self.send(every, every, 0, self.part, lambda: h.peer(3, 1))]
        start(self.flying)


class Gather:
    def __init__(self, here, lanes, block, shard, part, own=None):
        self.here, self.lanes, self.block, self.own = here, lanes, block, own
        y = here.y
        self.left, self.right, self.far = here.near[0][3], here.near[0][1], here.near[0][2]
        wide = 3 * WIDE
        lone = part - 2 * wide
        quarter, eighth, mid = shard // 4, shard // 8, shard // 2
        cuts = ((lone, 2), (lone + wide, 1))
        self.pieces, self.relays = [], []
        for column, axis in cuts:
            me = here.co[axis] * quarter
            self.pieces += self.pair(y, y, me, me, quarter, column, wide, 0)
            self.relays += self.pair(
                self.left, self.right, me, me + eighth, eighth, column, wide, 0
            )
        self.lone = self.pair(y, y, 0, 0, shard, 0, lone, 0)
        self.lone_relay = self.pair(self.left, self.right, 0, mid, mid, 0, lone, 0)
        self.around, self.passed = {}, {}
        for n, s in (("left", self.left), ("right", self.right), ("far", self.far)):
            self.around[n], self.passed[n] = [], []
            for column, axis in cuts:
                me = here.co[axis] * quarter
                down, up = here.near[axis][3] * quarter, here.near[axis][1] * quarter
                self.around[n] += self.pair(s, s, me, me, quarter, column, wide, axis)
                self.passed[n] += self.pair(s, s, down, up + eighth, eighth, column, wide, axis)

    def pair(self, s_up, s_down, at_up, at_down, count, column, size, axis):
        def trip(s, at, step):
            def ends():
                src = dst = self.block(s, at, count, column, size)
                if self.own is not None and s is self.here.y:
                    src = self.own(at, count, column, size)
                return src, dst, self.here.peer(axis, step)

            return self.lanes.go(ends)

        return [trip(s_up, at_up, 1), trip(s_down, at_down, 3)]


def start(copies):
    for copy in copies:
        copy.start()


def arrive(copies):
    for copy in copies:
        copy.wait_recv()


def step_kernel(
    ids_ref, target_ref, mask_ref, gain_flat, hidden_ref, cot_ref, table_ref,
    grad_out, gain_out, head_out, emb_out, cot_all, cot_other, loss_ref, meta_out, marks_out, flags_out,
    table, norm, tall, pre, slope, wide, gain_ref, meta_mine, meta, id_col, scale, mine, slot_r, slot_f,
    low_send, low_own, low, slots0, slots1, slots2, low_tile_send, low_tile_recv, low_core_send, low_core_recv,
    crecv, gains, slot_g, acc, slots, grid, hidden_sums, tile_send, tile_recv,
    send_sem, recv_sem, core_send, core_recv, local_sem, out_sem,
):
    here = Here()
    y, z, x, c = here.y, here.z, here.x, here.c
    rows, width = table_ref.shape
    part = width // 2
    shard = hidden_ref.shape[0]
    tokens = SIDE * shard
    tiles = part // WIDE
    padded = table.shape[1]
    first_row = (y * 32 + here.v) * rows
    lanes = Lanes(send_sem, recv_sem)
    scatter = Scatter(here, low, (slots0, slots1, slots2), low_tile_send, low_tile_recv)

    hidden_load = pltpu.make_async_copy(hidden_ref, wide, local_sem.at[2])
    hidden_load.start()
    loads = [
        pltpu.make_async_copy(
            table_ref.at[:, pl.ds(h * part, part)], table.at[h, pl.ds(0, rows)], local_sem.at[h]
        )
        for h in (0, 1)
    ]
    for load in loads:
        load.start()
    row, face = here.row(), here.face(0, 1)
    row_at, face_at = x * 2 + c, y * SIDE + z
    entered = here.enter([p for i, p in enumerate(row) if i % 2 == 0 and i > 0], here.all_faces())

    for i, ref in enumerate((ids_ref, target_ref, mask_ref)):
        meta_mine[i : i + 1, :] = ref[...].reshape(1, shard)
    gain_ref[...] = gain_flat[...].reshape(1, width)
    meta[y] = meta_mine[...]
    own = of(y * shard, shard)

    hidden_load.wait()

    def normalize(i, carry):
        at = pl.ds(of(i * 64, 64), 64)
        full = wide[at, :].astype(F32)
        inv = lax.rsqrt(jnp.sum(full * full, axis=1, keepdims=True) / width + EPSILON)
        out = (full * inv * gain_ref[...]).astype(BF16)
        to = pl.ds(of(own + i * 64, 64), 64)
        norm[0, to, :] = out[:, :part]
        norm[1, to, :] = out[:, part:]
        return carry

    lax.fori_loop(0, shard // 64, normalize, 0)
    entered()
    meta_copies = [
        lanes.go(lambda s=s: (meta_mine, meta.at[y], here.peer(0, s))) for s in (1, 2, 3)
    ]
    for copy in meta_copies:
        copy.start()

    def norm_block(s, offset, count, column, size):
        return norm.at[c, pl.ds(of(s * shard + offset, 16), count), pl.ds(column, size)]

    normed = Gather(here, lanes, norm_block, shard, part)
    across = {
        n: lanes.go(
            lambda s=s: (
                norm_block(s, 0, shard, 0, part), norm_block(s, 0, shard, 0, part), here.peer(3, 1)
            )
        )
        for n, s in (("left", normed.left), ("right", normed.right), ("far", normed.far))
    }
    start(normed.pieces)
    for copy in meta_copies:
        copy.wait_recv()
    for s in range(SIDE):
        local = (meta[s, 0:1, :] - first_row).astype(F32)
        id_col[s * shard : (s + 1) * shard, :] = jnp.transpose(
            jnp.broadcast_to(local, (LANES, shard))
        ).astype(I32)

    def onehot(i, carry):
        at = pl.ds(of(i * 64, 64), 64)
        ids = id_col[at, :]
        lane = lax.broadcasted_iota(I32, (64, LANES), 1)
        for t in range(padded // LANES):
            inside = lane + t * LANES
            hit = ids == (jnp.where(inside < rows, inside, -1) if (t + 1) * LANES > rows else inside)
            tall[at, t * LANES : (t + 1) * LANES] = jnp.where(hit, 1.0, 0.0).astype(BF16)
        return carry

    lax.fori_loop(0, tokens // 64, onehot, 0)
    for h in (0, 1):
        table[h, rows:padded, :] = jnp.zeros((padded - rows, part), BF16)
    for load in loads:
        load.wait()

    def low_slot(j):
        at = (j // 4, j % 4) if isinstance(j, int) else (lax.div(j, 4), lax.rem(j, 4))
        return (pl.ds(of(at[0] * tokens, tokens), tokens), pl.ds(of(at[1] * WIDE, WIDE), WIDE))

    def low_copy(j):
        return pltpu.make_async_remote_copy(
            src_ref=low_send.at[odd(j)],
            dst_ref=slope.at[low_slot(j)],
            send_sem=low_core_send.at[j],
            recv_sem=low_core_recv.at[j],
            device_id=here.peer(3, 1),
        )

    blocks = (SIDE, SIDE, SIDE, 16, WIDE)

    def find(j, carry):
        columns = pl.ds(of(j * WIDE, WIDE), WIDE)

        def product(h):
            out = jnp.dot(tall[...], table[h, :, columns], preferred_element_type=F32)
            return out.astype(BF16)

        @pl.when(j >= 2)
        def _():
            low_copy(j - 2).wait_send()

        low_send[odd(j)] = product(1 - c)
        low[j] = product(c).reshape(blocks)
        low_copy(j).start()

        @pl.when(j == 1)
        def _():
            arrive(normed.pieces)
            start(normed.relays + normed.around["left"] + normed.around["right"] + normed.lone)

        @pl.when(j == 3)
        def _():
            arrive(normed.relays)
            start(normed.around["far"])

        @pl.when(j == 4)
        def _():
            arrive(normed.around["left"] + normed.around["right"])
            start(normed.passed["left"] + normed.passed["right"])
            arrive(normed.lone)
            start(normed.lone_relay)

        return carry

    soon = tiles - LATE
    lax.fori_loop(0, soon, find, 0)
    arrive(normed.around["far"])
    start(normed.passed["far"])
    arrive(normed.passed["left"] + normed.passed["right"])
    start([across["left"], across["right"]])
    arrive(normed.lone_relay + normed.passed["far"])
    across["far"].start()

    def found_start(some):
        for j in some:
            low_copy(j).wait_recv()
            low[j] = low[j] + slope[low_slot(j)].reshape(blocks)
            scatter.step(0, j, j % 3)

    found_start(range(soon))
    arrive(list(across.values()))
    group = 2 * shard
    tall_rows = rows // 5
    def target_of(g):
        both_rows = [meta[2 * g + i, 1:2, :] - first_row for i in (0, 1)]
        row = jnp.concatenate(both_rows, axis=1)
        return jnp.where((row >= 0) & (row < rows), row, -1)

    def weight_of(g):
        return jnp.concatenate([meta[2 * g + i, 2:3, :] for i in (0, 1)], axis=1).astype(F32)

    def found_step(k, some=range(soon)):
        for j in some:
            scatter.step(k, j, j % 3)

    def emit():
        for j in range(tiles):
            found = low[j, y, z, x].astype(F32) * math.sqrt(width)
            low_own[:, j * WIDE : (j + 1) * WIDE] = found.astype(BF16)

    emb_local = pltpu.make_async_copy(
        low_own, emb_out.at[z, x, :, pl.ds(of(c * part, LANES), part)], local_sem.at[3]
    )
    emb_spread = Spread(here, lanes, emb_out)

    def cot_block(s, offset, count, column, size):
        return cot_all.at[pl.ds(of(s * shard + offset, 16), count), pl.ds(column, size)]

    def cot_own(offset, count, column, size):
        at = pl.ds(of(offset, 16), count)
        return cot_ref.at[at, pl.ds(of(c * part + column, LANES), size)]

    gather = Gather(here, lanes, cot_block, shard, part, cot_own)
    across = [
        lanes.go(
            lambda s=s: (
                cot_all.at[pl.ds(of(s * shard, 16), shard)],
                cot_other.at[pl.ds(of(s * shard, 16), shard)],
                here.peer(3, 1),
            )
        )
        for s in (gather.left, gather.right, gather.far)
    ]
    def cot_first():
        arrive(gather.pieces)
        start(gather.relays + gather.around["left"] + gather.around["right"] + gather.lone)

    def cot_far():
        arrive(gather.relays)
        start(gather.around["far"])

    def cot_pass():
        arrive(gather.around["left"] + gather.around["right"] + gather.lone)
        start(gather.passed["left"] + gather.passed["right"] + gather.lone_relay)

    def cot_last():
        arrive(gather.around["far"])
        start(gather.passed["far"])

    def cot_done():
        arrive(gather.passed["left"] + gather.passed["right"] + gather.passed["far"])
        arrive(gather.lone_relay)
        start(across)

    acts = {
        "f1": lambda: found_step(1),
        "f2": lambda: found_step(2),
        "f3": lambda: found_step(3),
        "g1": lambda: found_step(1, range(soon, tiles)),
        "g2": lambda: found_step(2, range(soon, tiles)),
        "g3": lambda: (found_step(3, range(soon, tiles)), emit(), emb_local.start()),
        "e0": lambda: (emb_local.wait(), emb_spread.step(0)),
        "e1": lambda: emb_spread.step(1),
        "e2": lambda: emb_spread.step(2),
        "c0": lambda: start(gather.pieces),
        "c1": cot_first,
        "c2": cot_far,
        "c3": cot_pass,
        "c4": cot_last,
        "c5": cot_done,
    }

    def moves(stage):
        out = {}
        for name, (at, i) in MOVES.items():
            if at == stage:
                out.setdefault(i, []).append(acts[name])
        return out

    def move(table_of, i):
        for act in table_of[i]:
            act()

    plan = moves(0)

    def exchange_start(g, stage):
        me, slots = ((row_at, slot_r), (face_at, slot_f))[stage]
        peers = (row, face)[stage]
        slots[g, me] = mine[g, stage]
        out = [
            lanes.go(lambda p=p: (mine.at[g, stage], slots.at[g, me], p)) for p in peers
        ]
        start(out)
        return out

    def exchange_step(g, stage, flying):
        arrive(flying)
        slots = (slot_r, slot_f)[stage - 1]
        parts = [slots[g, i] for i in range(slots.shape[1])]
        while len(parts) > 1:
            parts = [a + b for a, b in zip(parts[::2], parts[1::2])]
        mine[g, stage] = parts[0]
        return exchange_start(g, stage) if stage < 2 else []

    flights = {}
    targets = [target_of(g) for g in (0, 1)]
    zero = jnp.zeros((8, group), F32)

    def logits(g, r):
        token_at = slice(g * group, (g + 1) * group)
        at = pl.ds(of(r * tall_rows, 16), tall_rows)
        raw = [
            lax.dot_general(
                table[h, at, :], norm[h, token_at, :],
                (((1,), (1,)), ((), ())), preferred_element_type=F32,
            )
            for h in (0, 1)
        ]
        pre[at, token_at] = raw[0] + raw[1]

    def shape(g, r, sums):
        token_at = slice(g * group, (g + 1) * group)
        total, picked = sums
        fold = lambda a: jnp.sum(a.reshape(5, 8, group), axis=0)
        for i in range(tall_rows // 40):
            at = pl.ds(of(r * tall_rows + i * 40, 8), 40)
            bent = jnp.tanh(pre[at, token_at] * (1.0 / SOFTCAP))
            grown = jnp.exp(bent * SOFTCAP)
            pre[at, token_at] = grown * (1.0 - bent * bent)
            ids = lax.broadcasted_iota(I32, bent.shape, 0) + (r * tall_rows + i * 40)
            total = total + fold(grown)
            picked = picked + fold(jnp.where(ids == targets[g], bent, 0.0))
        return total, picked

    def onward(g, r):
        for k in plan:
            if k // 5 == g:

                @pl.when(r == k % 5)
                def _(k=k):
                    move(plan, k)

        if g == 1:
            for i in (1, 2):

                @pl.when(r == 2 * i)
                def _(i=i):
                    flights[0] = exchange_step(0, i, flights[0])

    def post(g, sums):
        total, picked = [jnp.sum(a, axis=0, keepdims=True) for a in sums]
        for i in range(group // LANES):
            mine[g, 0, i : i + 1, :] = total[:, i * LANES : (i + 1) * LANES]
            mine[g, 0, 4 + i : 5 + i, :] = picked[:, i * LANES : (i + 1) * LANES]
        flights[g] = exchange_start(g, 0)

    for g in (0, 1):
        if g == 1:
            sums_0 = shape(0, 4, sums_0)
        logits(g, 0)
        if g == 1:
            post(0, sums_0)
        if 5 * g in plan:
            move(plan, 5 * g)

        def both(r, sums, g=g):
            sums = shape(g, r - 1, sums)
            logits(g, r)
            onward(g, r)
            return sums

        sums_0 = lax.fori_loop(1, 5, both, (zero, zero))
    post(1, shape(1, 4, sums_0))

    pre[rows:padded, :] = jnp.zeros((padded - rows, tokens), F32)
    sums = []

    def slopes(g):
        target, weight = target_of(g), weight_of(g)
        stats = mine[g, 2]
        lines = [jnp.concatenate([stats[i + 4 * k : i + 4 * k + 1] for i in range(4)], axis=1) for k in (0, 1)]
        total, bent = lines
        chosen = jnp.exp(bent * SOFTCAP) / total
        sums.append(
            (
                jnp.sum(weight * (jnp.log(total) - SOFTCAP * bent), axis=1, keepdims=True),
                jnp.sum(weight, axis=1, keepdims=True),
            )
        )
        bound = 0.17 * (jnp.maximum(1.0 - chosen, 0.0) + 1e-5)
        scale[g * group : (g + 1) * group, :] = jnp.transpose(
            jnp.broadcast_to(bound, (LANES, group))
        )
        factor = weight / total
        drop = weight * (1.0 - bent * bent)

        def turn(i, carry):
            at = pl.ds(of(i * WIDE, WIDE), WIDE)
            ids = lax.broadcasted_iota(I32, (WIDE, shard), 0) + i * WIDE
            for s in (0, 1):
                here_at = slice(g * group + s * shard, g * group + (s + 1) * shard)
                cut = slice(s * shard, (s + 1) * shard)
                value = pre[at, here_at] * factor[:, cut]
                value = value - jnp.where(ids == target[:, cut], drop[:, cut], 0.0)
                low = value.astype(BF16)
                slope[at, here_at] = low
                tall[here_at, at] = jnp.transpose(low)
            return carry

        lax.fori_loop(0, padded // WIDE, turn, 0)
    places = lax.broadcasted_iota(I32, (64, shard), 1)

    def earlier(i, carry):
        at = pl.ds(of(i * 64, 64), 64)
        token = lax.broadcasted_iota(I32, (64, shard), 0) + i * 64
        ids = jnp.concatenate([id_col[at, :]] * (shard // LANES), axis=1)
        out = []
        for s in range(SIDE):
            same = ids == meta[s, 0:1, :] - first_row
            again = jnp.where(same & (token < places + s * shard), 1.0, 0.0)
            out.append(carry[s] + jnp.sum(again.reshape(8, 8, shard), axis=0))
        return tuple(out)

    repeats = lax.fori_loop(0, tokens // 64, earlier, (jnp.zeros((8, shard), F32),) * SIDE)
    lines = []
    for s in range(SIDE):
        local = meta[s, 0:1, :] - first_row
        fresh = jnp.sum(repeats[s], axis=0, keepdims=True) == 0.0
        marked = (local >= 0) & (local < rows) & fresh
        lines.append(jnp.where(marked, 1.0, 0.0))
        marks_out[s : s + 1, :] = jnp.where(marked, local + 1, 0)
    stacked = jnp.concatenate(lines + [jnp.zeros((8 - SIDE, shard), F32)], axis=0)
    member = lax.div(lax.broadcasted_iota(I32, (shard, LANES), 0), 16)
    member = jnp.where(member == lax.broadcasted_iota(I32, (shard, LANES), 1), 1.0, 0.0)
    flags_out[...] = jnp.dot(
        stacked.astype(BF16), member.astype(BF16), preferred_element_type=F32
    ).astype(I32)
    lax.fori_loop(soon, tiles, find, 0)
    flights[1] = exchange_step(1, 1, flights[1])
    found_start(range(soon, tiles))
    slopes(0)
    flights[1] = exchange_step(1, 2, flights[1])
    slopes(1)
    loss = (sums[0][0] + sums[1][0]) / jnp.maximum(sums[0][1] + sums[1][1], 1.0)
    loss_ref[0, 0] = loss[0, 0]
    meta_out[...] = meta[...]
    reduce = Reduce(here, acc, slots, grid, hidden_sums, tile_send, tile_recv)

    def other_at(j):
        return (pl.ds(tokens, tokens), pl.ds(of(odd(j) * WIDE, WIDE), WIDE))

    def fourth(j):
        return j % 4 if isinstance(j, int) else lax.rem(j, 4)

    def core_copy(j):
        return pltpu.make_async_remote_copy(
            src_ref=pre.at[other_at(j)],
            dst_ref=crecv.at[fourth(j)],
            send_sem=core_send.at[j],
            recv_sem=core_recv.at[j],
            device_id=here.peer(3, 1),
        )

    delays = DELAYS

    def substeps(s):
        for k in range(4):
            j = s - delays[k]

            @pl.when((j >= 0) & (j < tiles))
            def _(k=k, j=j):
                if k == 0:
                    core_copy(j).wait_recv()

                    def fit(i, carry):
                        at = pl.ds(of(i * shard, shard), shard)
                        factor = FULL / scale[at, :]
                        total = pre[at, pl.ds(of(third(j) * WIDE, WIDE), WIDE)] + crecv[fourth(j), at, :]
                        total = total * jnp.concatenate([factor] * (WIDE // LANES), axis=1)
                        whole = jnp.round(total).astype(I32).astype(I16)
                        acc[j, i] = whole.reshape(blocks[1:])
                        return carry

                    lax.fori_loop(0, SIDE, fit, 0)
                for o in range(3):

                    @pl.when(lax.rem(j, 3) == o)
                    def _(o=o):
                        reduce.step(k, j, o)

    def tile(j, carry):
        columns = pl.ds(of(j * WIDE, WIDE), WIDE)

        def product(h):
            return jnp.dot(tall[...], table[h, :, columns], preferred_element_type=F32)

        @pl.when(j >= 2)
        def _():
            core_copy(j - 2).wait_send()

        pre[other_at(j)] = product(1 - c)
        pre[0:tokens, pl.ds(of(third(j) * WIDE, WIDE), WIDE)] = product(c)
        core_copy(j).start()
        substeps(j)
        for i in turns:

            @pl.when(j == i)
            def _(i=i):
                move(turns, i)

        return carry

    turns = moves(1)
    lax.fori_loop(0, tiles, tile, 0)
    def head_copy(j, h):
        return pltpu.make_async_copy(
            table.at[h, pl.ds(0, rows), pl.ds(of(j * WIDE, WIDE), WIDE)],
            head_out.at[:, pl.ds(of(h * part + j * WIDE, LANES), WIDE)],
            out_sem.at[h, j],
        )

    spans = [
        (h, j, slice(h * part + j * WIDE, h * part + (j + 1) * WIDE))
        for h in (0, 1)
        for j in range(tiles)
    ]

    def upstream(h, j, i):
        unit = scale[pl.ds(of(y * shard + i * 64, 64), 64), 0:1] * (1.0 / FULL)
        return hidden_sums[h, j, i].reshape(64, WIDE).astype(I32).astype(F32) * unit

    def reduce_rows(i, carry):
        at = pl.ds(of(i * 64, 64), 64)
        square = jnp.zeros((64, WIDE), F32)
        dot = jnp.zeros((64, WIDE), F32)
        for h, j, cols in spans:
            hidden = wide[at, cols].astype(F32)
            square = square + hidden * hidden
            dot = dot + (upstream(h, j, i) * gain_ref[:, cols]) * hidden
        inv = lax.rsqrt(jnp.sum(square, axis=1, keepdims=True) / width + EPSILON)
        back = (inv * inv * inv) * (jnp.sum(dot, axis=1, keepdims=True) / width)
        crecv[0, at, 0:LANES] = jnp.broadcast_to(inv, (64, LANES))
        crecv[0, at, LANES : 2 * LANES] = jnp.broadcast_to(back, (64, LANES))
        for h, j, cols in spans:
            each = jnp.sum(upstream(h, j, i) * wide[at, cols].astype(F32) * inv, axis=0, keepdims=True)
            line = (h * part + j * WIDE) // LANES
            for q in range(WIDE // LANES):
                to = slice(line + q, line + q + 1)
                gains[to, :] = gains[to, :] + each[:, q * LANES : (q + 1) * LANES]
        return carry

    def gradient(i, carry):
        at = pl.ds(of(i * 64, 64), 64)
        inv = crecv[0, at, 0:1]
        back = crecv[0, at, LANES : LANES + 1]
        for h, j, cols in spans:
            hidden = wide[at, cols].astype(F32)
            raw = upstream(h, j, i)
            wide[at, cols] = (inv * (raw * gain_ref[:, cols]) - hidden * back).astype(BF16)
        return carry

    later = moves(2)

    def head(j, carry):
        columns = pl.ds(of(j * WIDE, WIDE), WIDE)
        for i in range(5):
            at = slice(i * rows // 5, (i + 1) * rows // 5)
            both = [
                jnp.dot(slope[at, :], norm[h, :, columns], preferred_element_type=F32)
                for h in (0, 1)
            ]
            for h in (0, 1):
                table[h, at, columns] = both[h].astype(BF16)
        for h in (0, 1):
            head_copy(j, h).start()
        substeps(j + tiles)
        for i in later:

            @pl.when(j == i)
            def _(i=i):
                move(later, i)

        return carry

    lax.fori_loop(0, tiles, head, 0)
    for s in range(2 * tiles, tiles + DELAYS[3]):
        for k in range(4):
            j = s - DELAYS[k]
            if 0 <= j < tiles:
                reduce.step(k, j, j % 3)
    last = moves(3)
    for i in sorted(last):
        move(last, i)
    gains[...] = jnp.zeros(gains.shape, F32)
    for j in range(tiles):
        reduce.step(4, j, j % 3)
    lax.fori_loop(0, SIDE, reduce_rows, 0)
    slot_g[y] = gains[...]
    gain_copies = [
        lanes.go(lambda s=s: (gains, slot_g.at[y], here.offset({0: s}))) for s in (1, 2, 3)
    ]
    start(gain_copies)
    lax.fori_loop(0, SIDE, gradient, 0)
    grad_copy = pltpu.make_async_copy(wide, grad_out, local_sem.at[1])
    grad_copy.start()
    for j in range(tiles):
        for h in (0, 1):
            head_copy(j, h).wait()
    arrive(across)
    arrive(gain_copies)
    lines = gain_out.shape[0]
    gain_out[...] = ((slot_g[0] + slot_g[1]) + (slot_g[2] + slot_g[3]))[0:lines]
    grad_copy.wait()
    arrive(emb_spread.flying)
    for copy in lanes.made:
        if copy.gone:
            copy.wait_send()
    for j in range(tiles):
        if j >= tiles - 2:
            core_copy(j).wait_send()
            low_copy(j).wait_send()
        scatter.drain(j, j % 3)
        reduce.drain(j, j % 3)


def finish_kernel(
    mark_ref, flag_ref, row_ref, head_ref, emb_ref, grad_ref, gain_ref, cot_ref, half_ref, other_ref,
    head_out, emb_out, grad_out, gain_out,
    tall, short, cots, ones, sums, found, touched, count, came, left, cot_sem,
):
    y, v = lax.axis_index("dp"), lax.axis_index("vocab")
    c = lax.rem(v, 2)
    rows, width = head_ref.shape
    shard, part = cot_ref.shape[0], width // 2
    first_row = (y * 32 + v) * rows
    batch = ones.shape[0]
    step = rows // BLOCKS

    def into(k):
        at = pl.ds(of(k * step, step), step)
        return pltpu.make_async_copy(head_ref.at[at], tall.at[at], came.at[k])

    def out(k):
        at = pl.ds(of(k * step, step), step)
        return pltpu.make_async_copy(tall.at[at], head_out.at[at], left.at[k])

    small_in = [
        pltpu.make_async_copy(src, short.at[k], came.at[BLOCKS + k])
        for k, src in enumerate((emb_ref, grad_ref))
    ]
    small_out = [
        pltpu.make_async_copy(short.at[k], dst, left.at[BLOCKS + k])
        for k, dst in enumerate((emb_out, grad_out))
    ]
    cot_copies = [
        pltpu.make_async_copy(cot_ref, cots.at[pl.ds(of(y * shard, shard), shard)], cot_sem.at[0])
    ]
    for i in (1, 2, 3):
        at = pl.ds(of(lax.rem(y + i, SIDE) * shard, shard), shard)
        for k, (src, h) in enumerate(((half_ref, c), (other_ref, 1 - c))):
            cot_copies.append(
                pltpu.make_async_copy(
                    src.at[at], cots.at[at, pl.ds(of(h * part, LANES), part)],
                    cot_sem.at[2 * i - 1 + k],
                )
            )
    start(cot_copies)
    for k in range(BLOCKS):
        touched[k] = 0
        into(k).start()
    start(small_in)
    gain_out[...] = gain_ref[...]

    count[0] = 0
    for s in range(SIDE):

        def look(i, carry, s=s):
            @pl.when(flag_ref[s, i] > 0)
            def _():
                for k in range(16):
                    t = i * 16 + k

                    @pl.when(mark_ref[s, t] > 0)
                    def _(t=t):
                        row = mark_ref[s, t] - 1
                        found[count[0]] = row
                        count[0] = count[0] + 1
                        touched[lax.div(row, step)] = 1

            return carry

        lax.fori_loop(0, shard // 16, look, 0)
    total = count[0]
    ids = jnp.concatenate([row_ref[s, 0:1, :] for s in range(SIDE)], axis=1) - first_row
    for copy in cot_copies:
        copy.wait()

    def pass_on(k, carry):
        into(k).wait()

        @pl.when(touched[k] == 0)
        def _():
            out(k).start()

        return carry

    def mark_rows(b):
        size = jnp.minimum(total - b * batch, batch)
        ones[...] = jnp.zeros(ones.shape, F32)

        def mark(u, carry):
            ones[pl.ds(u, 1), :] = jnp.where(ids == found[b * batch + u], 1.0, 0.0)
            return carry

        lax.fori_loop(0, size, mark, 0)
        low = ones[...].astype(BF16)

        def product(j, carry):
            columns = pl.ds(of(j * 512, 512), 512)
            sums[:, columns] = jnp.dot(low, cots[:, columns], preferred_element_type=F32)
            return carry

        lax.fori_loop(0, width // 512, product, 0)
        return size

    def add_rows(b, size):
        def place(u, carry):
            row = found[b * batch + u]
            at = pl.ds(of(lax.div(row, 16) * 16, 16), 16)
            chosen = lax.broadcasted_iota(I32, (16, width), 0) == lax.rem(row, 16)
            more = jnp.where(chosen, sums[pl.ds(u, 1), :] * math.sqrt(width), 0.0)
            tall[at, :] = (tall[at, :].astype(F32) + more).astype(BF16)
            return carry

        lax.fori_loop(0, size, place, 0)

    size = mark_rows(0)
    lax.fori_loop(0, BLOCKS, pass_on, 0)
    add_rows(0, size)

    def add_batch(b, carry):
        add_rows(b, mark_rows(b))
        return carry

    lax.fori_loop(1, lax.div(total + batch - 1, batch), add_batch, 0)

    def send_rest(k, carry):
        @pl.when(touched[k] != 0)
        def _():
            out(k).start()

        return carry

    lax.fori_loop(0, BLOCKS, send_rest, 0)
    for copy, next_copy in zip(small_in, small_out):
        copy.wait()
        next_copy.start()

    def settle(k, carry):
        out(k).wait()
        return carry

    lax.fori_loop(0, BLOCKS, settle, 0)
    for copy in small_out:
        copy.wait()


def finish(tables, meta, head, embedded, grad, gain, cotangent, cot_half, cot_other):
    rows, width = head.shape
    tokens = cot_half.shape[0]
    any_ = pl.BlockSpec(memory_space=pl.ANY)
    smem, vmem = pl.BlockSpec(memory_space=pltpu.SMEM), pl.BlockSpec(memory_space=pltpu.VMEM)
    results = (head, embedded, grad, gain)
    return pl.pallas_call(
        finish_kernel,
        out_shape=tuple(jax.ShapeDtypeStruct(a.shape, a.dtype) for a in results),
        in_specs=[smem] * 2 + [vmem] + [any_] * 3 + [vmem] + [any_] * 3,
        out_specs=(any_, any_, any_, vmem),
        scratch_shapes=[
            pltpu.VMEM(head.shape, BF16),
            pltpu.VMEM((2, *grad.shape), BF16),
            pltpu.VMEM((tokens, width), BF16),
            pltpu.VMEM((64, tokens), F32),
            pltpu.VMEM((64, width), F32),
            pltpu.SMEM((tokens,), I32),
            pltpu.SMEM((BLOCKS,), I32),
            pltpu.SMEM((1,), I32),
            pltpu.SemaphoreType.DMA((BLOCKS + 2,)),
            pltpu.SemaphoreType.DMA((BLOCKS + 2,)),
            pltpu.SemaphoreType.DMA((7,)),
        ],
        compiler_params=pltpu.CompilerParams(vmem_limit_bytes=63 * 1024 * 1024),
    )(*tables, meta, head, embedded, grad, gain, cotangent, cot_half, cot_other)


def body(input_ids, target_ids, loss_mask, final_hidden, norm_gain, embed_cotangent, table):
    rows, width = table.shape
    shard = final_hidden.shape[0]
    tokens, part = SIDE * shard, width // 2
    tiles = part // WIDE
    padded = -(-rows // WIDE) * WIDE
    any_ = pl.BlockSpec(memory_space=pl.ANY)
    vmem = pl.BlockSpec(memory_space=pltpu.VMEM)
    smem = pl.BlockSpec(memory_space=pltpu.SMEM)
    dma = pltpu.SemaphoreType.DMA
    share = (SIDE, SIDE, 16)
    blocks = (SIDE, SIDE, SIDE, 16, WIDE)
    grad, gain, head, embedded, cot_half, cot_other, loss, meta_all, marks, flags = pl.pallas_call(
        step_kernel,
        out_shape=(
            jax.ShapeDtypeStruct((shard, width), BF16),
            jax.ShapeDtypeStruct((width // LANES, LANES), F32),
            jax.ShapeDtypeStruct((rows, width), BF16),
            jax.ShapeDtypeStruct((*share, width), BF16),
            jax.ShapeDtypeStruct((tokens, part), BF16),
            jax.ShapeDtypeStruct((tokens, part), BF16),
            jax.ShapeDtypeStruct((1, 1), F32),
            jax.ShapeDtypeStruct((SIDE, 8, shard), I32),
            jax.ShapeDtypeStruct((SIDE, shard), I32),
            jax.ShapeDtypeStruct((8, LANES), I32),
        ),
        in_specs=[vmem] * 4 + [any_] * 3,
        out_specs=(any_, vmem, any_, any_, any_, any_, smem, vmem, vmem, vmem),
        scratch_shapes=[
            pltpu.VMEM((2, padded, part), BF16),
            pltpu.VMEM((2, tokens, part), BF16),
            pltpu.VMEM((tokens, padded), BF16),
            pltpu.VMEM((padded, tokens), F32),
            pltpu.VMEM((padded, tokens), BF16),
            pltpu.VMEM((shard, width), BF16),
            pltpu.VMEM((1, width), F32),
            pltpu.VMEM((8, shard), I32),
            pltpu.VMEM((SIDE, 8, shard), I32),
            pltpu.VMEM((tokens, LANES), I32),
            pltpu.VMEM((tokens, LANES), F32),
            pltpu.VMEM((2, 3, 8, LANES), F32),
            pltpu.VMEM((2, 8, 8, LANES), F32),
            pltpu.VMEM((2, 16, 8, LANES), F32),
            pltpu.VMEM((2, tokens, WIDE), BF16),
            pltpu.VMEM((16, part), BF16),
            *scatter_scratch(tiles, BF16),
            dma((tiles,)), dma((tiles,)),
            pltpu.VMEM((4, tokens, WIDE), F32),
            pltpu.VMEM((32, LANES), F32),
            pltpu.VMEM((SIDE, 32, LANES), F32),
            *reduce_scratch(tiles, I16),
            dma((150,)), dma((150,)), dma((tiles,)), dma((tiles,)), dma((4,)),
            dma((2, tiles)),
        ],
        compiler_params=pltpu.CompilerParams(
            collective_id=1, has_side_effects=True, vmem_limit_bytes=VMEM_BYTES
        ),
    )(input_ids, target_ids, loss_mask, norm_gain, final_hidden, embed_cotangent, table)
    head, embedded, grad, gain = finish(
        (marks, flags),
        meta_all,
        head,
        embedded.reshape(shard, width),
        grad,
        gain,
        embed_cotangent,
        cot_half,
        cot_other,
    )
    return embedded, loss.reshape(()), grad, gain.reshape(width), head


def solution(mesh):
    placed = (
        P("dp"),
        P("dp"),
        P("dp"),
        P("dp", None),
        P(),
        P("dp", None),
        P(("dp", "vocab"), None),
    )
    return jax.shard_map(
        body,
        mesh=mesh,
        in_specs=placed,
        out_specs=(P("dp", None), P(), P("dp", None), P(), P(("dp", "vocab"), None)),
        check_vma=False,
    )
```
